32 devices in a mesh: tm: 16 (over z, y, x), space: 2 (over core).
Axes of the slice: x: 2, y: 2, z: 4, core: 2. Of those that a mesh axis runs over, the one named last changes fastest.
Arguments:
- links: float32 [2, 3, 3, 64, 8192], P(None, None, None, 'tm', 'space'), may hold values from -1 to 1, as said below
Outputs:
- ploop: float32 [2, 8192], P(None, ('space', 'tm'))
- loop_stats: float32 [3], replicated
The draws below stay inside these ranges and needn't reach their ends.
Inputs may be any that keep to these rules, and one draw needn't show every extreme that they name: `links`: every link matrix is special unitary.
All inputs are finite; a program needn't handle non-finite values.
Results may differ from the reference program's by a relative error of at most 0.00014.
Values sent between devices are 32-bit elements; how exact they have to be, the bound alone decides.
A program may use at most 64 MiB of HBM per device.

```python
import jax
import jax.numpy as jnp
from jax import lax

NT = 64
NS = 8192


def inner_prod(first, second):
    real = jnp.sum(first[0] * second[0] + first[1] * second[1], axis=0)
    imag = jnp.sum(first[0] * second[1] - first[1] * second[0], axis=0)
    return (real, imag)


def unit_row(row):
    length = jnp.sqrt(jnp.maximum(jnp.sum(row[0] * row[0] + row[1] * row[1], axis=0), 1e-06))
    return row / length[None, None]


def draw_links(key, part):
    key_noise, key_size = jax.random.split(key)
    noise = jax.random.normal(key_noise, (2, 3, 3, NT, NS), jnp.float32)
    strength = jnp.exp(jax.random.uniform(key_size, (NT, NS), jnp.float32, jnp.log(0.05), jnp.log(0.3)))
    unit = jnp.stack([jnp.eye(3, dtype=jnp.float32), jnp.zeros((3, 3), jnp.float32)])
    matrix = unit[:, :, :, None, None] + noise * strength[None, None, None]
    first = unit_row(matrix[:, 0])
    second = matrix[:, 1]
    real, imag = inner_prod(first, second)
    second = jnp.stack([second[0] - (real * first[0] - imag * first[1]), second[1] - (real * first[1] + imag * first[0])])
    second = unit_row(second)

    def cross_part(j, k):
        real_part = first[0, j] * second[0, k] - first[1, j] * second[1, k] - (first[0, k] * second[0, j] - first[1, k] * second[1, j])
        imag_part = first[0, j] * second[1, k] + first[1, j] * second[0, k] - (first[0, k] * second[1, j] + first[1, k] * second[0, j])
        return (real_part, -imag_part)
    parts = [cross_part(1, 2), cross_part(2, 0), cross_part(0, 1)]
    third = jnp.stack([jnp.stack([p[0] for p in parts]), jnp.stack([p[1] for p in parts])])
    return jnp.stack([first, second, third], axis=1)


def setup_inputs(seed: int = 0) -> dict:
    key_of = jax.random.split(jax.random.key(seed), 2)
    links = draw_links(jax.random.fold_in(key_of[1], 71), 0)
    return {"links": links}


def cmul(left, right):
    def prod(first, second):
        return jnp.sum(first[:, :, None, :] * second[None, :, :, :], axis=1)
    return jnp.stack([prod(left[0], right[0]) - prod(left[1], right[1]),
                      prod(left[0], right[1]) + prod(left[1], right[0])])


def reference(links):
    def step(index, acc):
        return cmul(acc, lax.dynamic_index_in_dim(links, index, 3, keepdims=False))
    whole = lax.fori_loop(1, NT, step, links[:, :, :, 0, :])
    ploop = (whole[:, 0, 0] + whole[:, 1, 1] + whole[:, 2, 2]) / 3.0
    mean_re = jnp.sum(ploop[0]) / NS
    mean_im = jnp.sum(ploop[1]) / NS
    square = jnp.sum(ploop[0] * ploop[0] + ploop[1] * ploop[1]) / NS
    stats = jnp.stack([mean_re, mean_im, square - mean_re * mean_re - mean_im * mean_im])
    return ploop, stats
```

```python
import functools
import math

import jax
import jax.numpy as jnp
from jax import lax
from jax.experimental import pallas as pl
from jax.experimental.pallas import tpu as pltpu
from jax.sharding import PartitionSpec as P

MESH = pl.DeviceIdType.MESH
LANES = 128


def xor(index, flip):
    out, bit = 0, 1
    while bit <= flip:
        digit = index // bit % 2
        out = out + (bit * (1 - digit) if flip & bit else bit * digit)
        bit *= 2
    return out + index // bit * bit


def cmul(a, b):
    return (a[0] * b[0] - a[1] * b[1], a[0] * b[1] + a[1] * b[0])


def times(left, right):
    out = []
    for row in left:
        new = []
        for k in range(3):
            terms = [cmul(row[j], right[j][k]) for j in range(3)]
            new.append((terms[0][0] + terms[1][0] + terms[2][0], terms[0][1] + terms[1][1] + terms[2][1]))
        out.append(new)
    return out


def whole(rows):
    first, second = rows
    third = []
    for k in range(3):
        i, j = (k + 1) % 3, (k + 2) % 3
        p, q = cmul(first[i], second[j]), cmul(first[j], second[i])
        third.append((p[0] - q[0], q[1] - p[1]))
    return [first, second, third]


def take(block, rows):
    return [[(block[i * 3 + j], block[(rows + i) * 3 + j]) for j in range(3)] for i in range(rows)]


def flat(rows):
    return [x[part] for part in range(2) for row in rows for x in row]


def product(parts):
    while len(parts) > 1:
        merged = [times(parts[n], whole(parts[n + 1])) for n in range(0, len(parts) - 1, 2)]
        parts = merged + parts[2 * len(merged):]
    return parts[0]


def kernel(tm, space, low, high, nt, rows, share, total_sites,
           links, ploop, stats,
           staged, send1, recv1, send2, recv2, mine, others,
           in_sem, send_sem1, recv_sem1, send_sem2, recv_sem2, send_sem3, recv_sem3):
    me_tm, me_space = lax.axis_index("tm"), lax.axis_index("space")
    lo, hi = me_tm % low, me_tm // low
    me = me_tm * space + me_space
    count = tm * space
    band = high * rows

    def chunk_copies(slot, target):
        return [
            pltpu.make_async_copy(
                links.at[:, h, target], staged.at[slot, :, pl.ds(h * rows * nt, rows * nt), :], in_sem.at[slot]
            )
            for h in range(high)
        ]

    flips = [low - 1] + list(range(1, low - 1)) + [0] if low > 1 else [0]
    targets = [xor(lo, flip) for flip in flips]
    for slot, target in enumerate(targets):
        for copy in chunk_copies(slot, target):
            copy.start()

    barrier = pltpu.get_barrier_semaphore()

    def greet(step, carry):
        other = (me + step) % count
        pl.semaphore_signal(barrier, inc=1, device_id=(other // space, other % space), device_id_type=MESH)
        return carry

    lax.fori_loop(1, count, greet, 0, unroll=count <= 64)

    sends1 = []
    for slot, target in enumerate(targets):
        pltpu.make_async_copy(staged.at[slot], staged.at[slot], in_sem.at[slot]).wait()

        def matrix(t, count_rows):
            block = {}
            for part in range(2):
                for i in range(count_rows):
                    for j in range(3):
                        block[(part * count_rows + i) * 3 + j] = staged[
                            slot, part * 9 + i * 3 + j, pl.ds(t, band, stride=nt), :
                        ]
            return take(block, count_rows)

        acc = matrix(0, 2)
        for t in range(1, nt):
            acc = times(acc, matrix(t, 3))
        own = slot == len(targets) - 1
        for c, value in enumerate(flat(acc)):
            if own:
                recv1[lo, c] = value
            else:
                send1[slot, c] = value
        if slot == 0:
            pl.semaphore_wait(barrier, count - 1)
        if not own:
            copy = pltpu.make_async_remote_copy(
                src_ref=send1.at[slot], dst_ref=recv1.at[lo],
                send_sem=send_sem1.at[slot], recv_sem=recv_sem1.at[slot],
                device_id=(hi * low + target, me_space), device_id_type=MESH,
            )
            copy.start()
            sends1.append(copy)
    for copy in sends1:
        copy.wait_recv()

    acc = product([take([recv1[src, c] for c in range(12)], 2) for src in range(low)])
    for c, value in enumerate(flat(acc)):
        for h in range(high):
            send2[h, c] = value[h * rows:(h + 1) * rows, :]

    own2 = send2.at[hi]
    sends2 = []
    flips2 = list(range(high - 1, 0, -1))
    for slot, flip in enumerate(flips2):
        target = xor(hi, flip)
        copy = pltpu.make_async_remote_copy(
            src_ref=send2.at[target], dst_ref=recv2.at[hi],
            send_sem=send_sem2.at[slot], recv_sem=recv_sem2.at[slot],
            device_id=(target * low + lo, me_space), device_id_type=MESH,
        )
        copy.start()
        sends2.append(copy)
    for c in range(12):
        recv2[hi, c] = own2[c]
    for copy in sends2:
        copy.wait_recv()

    parts = [take([recv2[src, c] for c in range(12)], 2) for src in range(high)]
    half = max(high // 2, 1)
    left = whole(product(parts[:half]))
    if high > 1:
        right = whole(product(parts[half:]))
        terms = [cmul(left[i][j], right[j][i]) for i in range(3) for j in range(3)]
    else:
        terms = [left[i][i] for i in range(3)]
    re = functools.reduce(jnp.add, [x[0] for x in terms]) / 3.0
    im = functools.reduce(jnp.add, [x[1] for x in terms]) / 3.0
    mine[0:1, :] = jnp.sum(re, axis=0, keepdims=True)
    mine[1:2, :] = jnp.sum(im, axis=0, keepdims=True)
    mine[2:3, :] = jnp.sum(re * re + im * im, axis=0, keepdims=True)
    mine[3:4, :] = jnp.zeros((1, LANES), jnp.float32)

    def spread(step, carry):
        other = (me + step) % count
        pltpu.make_async_remote_copy(
            src_ref=mine, dst_ref=others.at[step - 1], send_sem=send_sem3, recv_sem=recv_sem3,
            device_id=(other // space, other % space), device_id_type=MESH,
        ).start()
        return carry

    lax.fori_loop(1, count, spread, 0, unroll=count <= 64)
    for r in range(rows):
        width = min(LANES, share - r * LANES)
        if width > 0:
            ploop[0:1, r * LANES:r * LANES + width] = re[r:r + 1, :width]
            ploop[1:2, r * LANES:r * LANES + width] = im[r:r + 1, :width]
    for copy in sends1 + sends2:
        copy.wait_send()
    pltpu.make_async_copy(others, others, recv_sem3).wait()
    sums = jnp.sum(others[...], axis=0) + mine[...]
    mean_re = jnp.sum(sums[0:1, :]) / total_sites
    mean_im = jnp.sum(sums[1:2, :]) / total_sites
    square = jnp.sum(sums[2:3, :]) / total_sites
    stats[0] = mean_re
    stats[1] = mean_im
    stats[2] = square - mean_re * mean_re - mean_im * mean_im
    pltpu.make_async_copy(others, others, send_sem3).wait()


def on_device(tm, space, links):
    nt, sites = links.shape[3], links.shape[4]
    share = sites // tm
    unit = LANES * (8 // math.gcd(8, nt))
    padded = -(-share // unit) * unit
    rows = padded // LANES
    low = 1 << (tm.bit_length() - 1) // 2
    high = tm // low
    view = links.reshape(18, nt, tm, share)
    if padded != share:
        view = jnp.pad(view, ((0, 0), (0, 0), (0, 0), (0, padded - share)))
    view = view.reshape(18, nt, tm * rows, LANES).transpose(0, 2, 1, 3)
    view = view.reshape(18, high, low, rows * nt, LANES)
    band = high * rows
    count = tm * space
    f32 = jnp.float32
    peers1, peers2 = max(low - 1, 1), max(high - 1, 1)
    return pl.pallas_call(
        functools.partial(kernel, tm, space, low, high, nt, rows, share, sites * space),
        out_shape=(jax.ShapeDtypeStruct((2, share), f32), jax.ShapeDtypeStruct((3,), f32)),
        in_specs=[pl.BlockSpec(memory_space=pl.ANY)],
        out_specs=(pl.BlockSpec(memory_space=pltpu.VMEM), pl.BlockSpec(memory_space=pltpu.SMEM)),
        scratch_shapes=[
            pltpu.VMEM((low, 18, band * nt, LANES), f32),
            pltpu.VMEM((peers1, 12, band, LANES), f32),
            pltpu.VMEM((low, 12, band, LANES), f32),
            pltpu.VMEM((high, 12, rows, LANES), f32),
            pltpu.VMEM((high, 12, rows, LANES), f32),
            pltpu.VMEM((4, LANES), f32),
            pltpu.VMEM((count - 1, 4, LANES), f32),
            pltpu.SemaphoreType.DMA((low,)),
            pltpu.SemaphoreType.DMA((peers1,)),
            pltpu.SemaphoreType.DMA((peers1,)),
            pltpu.SemaphoreType.DMA((peers2,)),
            pltpu.SemaphoreType.DMA((peers2,)),
            pltpu.SemaphoreType.DMA,
            pltpu.SemaphoreType.DMA,
        ],
        compiler_params=pltpu.CompilerParams(collective_id=0, has_side_effects=True),
    )(view)


def solution(mesh):
    return jax.shard_map(
        functools.partial(on_device, mesh.shape["tm"], mesh.shape["space"]),
        mesh=mesh,
        in_specs=(P(None, None, None, "tm", "space"),),
        out_specs=(P(None, ("space", "tm")), P()),
        check_vma=False,
    )
```

```python
import functools
import math

import jax
import jax.numpy as jnp
from jax import lax
from jax.experimental import pallas as pl
from jax.experimental.pallas import tpu as pltpu
from jax.sharding import PartitionSpec as P

MESH = pl.DeviceIdType.MESH
LANES = 128


def xor(index, flip):
    out, bit = 0, 1
    while bit <= flip:
        digit = index // bit % 2
        out = out + (bit * (1 - digit) if flip & bit else bit * digit)
        bit *= 2
    return out + index // bit * bit


def cmul(a, b):
    return (a[0] * b[0] - a[1] * b[1], a[0] * b[1] + a[1] * b[0])


def times(left, right):
    out = []
    for row in left:
        new = []
        for k in range(3):
            terms = [cmul(row[j], right[j][k]) for j in range(3)]
            new.append((terms[0][0] + terms[1][0] + terms[2][0], terms[0][1] + terms[1][1] + terms[2][1]))
        out.append(new)
    return out


def whole(rows):
    first, second = rows
    third = []
    for k in range(3):
        i, j = (k + 1) % 3, (k + 2) % 3
        p, q = cmul(first[i], second[j]), cmul(first[j], second[i])
        third.append((p[0] - q[0], q[1] - p[1]))
    return [first, second, third]


def take(block, rows):
    return [[(block[i * 3 + j], block[(rows + i) * 3 + j]) for j in range(3)] for i in range(rows)]


def flat(rows):
    return [x[part] for part in range(2) for row in rows for x in row]


def product(parts):
    while len(parts) > 1:
        merged = [times(parts[n], whole(parts[n + 1])) for n in range(0, len(parts) - 1, 2)]
        parts = merged + parts[2 * len(merged):]
    return parts[0]


def kernel(tm, space, low, high, nt, rows, share, total_sites,
           links, ploop, stats,
           staged, send1, recv1, send2, recv2, outbox, inbox, mine, others, shadow,
           in_sem, send_sem1, recv_sem1, send_sem2, recv_sem2, send_sem3, recv_sem3, send_sem4, recv_sem4):
    me_tm, me_space = lax.axis_index("tm"), lax.axis_index("space")
    lo, hi = me_tm % low, me_tm // low
    me = me_tm * space + me_space
    count = tm * space
    band = high * rows
    half = high // 2
    part = half * rows
    near = hi // half
    far = 1 - near
    order = (far, near)
    middles = (half - 1, half)
    voices = 2 * low * space

    def chunk_copies(slot, target):
        return [
            pltpu.make_async_copy(
                links.at[:, h, target], staged.at[slot, :, pl.ds(h * rows * nt, rows * nt), :], in_sem.at[slot]
            )
            for h in range(high)
        ]

    barrier = pltpu.get_barrier_semaphore()

    def greet(other_tm, other_space):
        pl.semaphore_signal(barrier, inc=1, device_id=(other_tm, other_space), device_id_type=MESH)

    for step in range(1, low):
        greet(hi * low + (lo + step) % low, me_space)
    for step in range(1, space):
        greet(me_tm, (me_space + step) % space)
    middle = (hi >= middles[0]) & (hi <= middles[1])

    @pl.when(middle)
    def _():
        for step in range(1, high):
            greet((hi + step) % high * low + lo, me_space)

    @pl.when(jnp.logical_not(middle))
    def _():
        for h in middles:
            greet(h * low + lo, me_space)

    flips = [low - 1] + list(range(1, low - 1)) + [0] if low > 1 else [0]
    targets = [xor(lo, flip) for flip in flips]
    for slot, target in enumerate(targets):
        for copy in chunk_copies(slot, target):
            copy.start()

    def send_half(slot, turn):
        copy = pltpu.make_async_remote_copy(
            src_ref=send1.at[slot, order[turn]], dst_ref=recv1.at[lo, order[turn]],
            send_sem=send_sem1.at[slot, turn], recv_sem=recv_sem1.at[slot, turn],
            device_id=(hi * low + targets[slot], me_space), device_id_type=MESH,
        )
        copy.start()
        return copy

    sends1 = ([], [])
    for slot, target in enumerate(targets):
        pltpu.make_async_copy(staged.at[slot], staged.at[slot], in_sem.at[slot]).wait()

        def matrix(t, count_rows):
            block = {}
            for p in range(2):
                for i in range(count_rows):
                    for j in range(3):
                        block[(p * count_rows + i) * 3 + j] = staged[
                            slot, p * 9 + i * 3 + j, pl.ds(t, band, stride=nt), :
                        ]
            return take(block, count_rows)

        acc = matrix(0, 2)
        for t in range(1, nt):
            acc = times(acc, matrix(t, 3))
        own = slot == len(targets) - 1
        for c, value in enumerate(flat(acc)):
            for k in range(2):
                if own:
                    recv1[lo, k, c] = value[k * part:(k + 1) * part, :]
                else:
                    send1[slot, k, c] = value[k * part:(k + 1) * part, :]
        if slot == 0:
            @pl.when(middle)
            def _():
                pl.semaphore_wait(barrier, low - 1 + space - 1 + high - 1)

            @pl.when(jnp.logical_not(middle))
            def _():
                pl.semaphore_wait(barrier, low - 1 + space - 1 + 2)
        if not own:
            sends1[0].append(send_half(slot, 0))
        if slot == len(targets) - 2:
            sends1[1].extend(send_half(k, 1) for k in range(len(targets) - 1))

    def send_product(turn):
        return pltpu.make_async_remote_copy(
            src_ref=send2.at[turn], dst_ref=recv2.at[hi],
            send_sem=send_sem2.at[turn], recv_sem=recv_sem2.at[hi],
            device_id=((half - 1 + order[turn]) * low + lo, me_space), device_id_type=MESH,
        )

    for turn in range(2):
        for copy in sends1[turn]:
            copy.wait_recv()
        acc = product([take([recv1[src, order[turn], c] for c in range(12)], 2) for src in range(low)])
        for c, value in enumerate(flat(acc)):
            send2[turn, c] = value
        if turn == 0:
            send_product(0).start()

    @pl.when(jnp.logical_not(middle))
    def _():
        send_product(1).start()

    def place(re, im):
        for r in range(rows):
            width = min(LANES, share - r * LANES)
            if width > 0:
                ploop[0:1, r * LANES:r * LANES + width] = re[r:r + 1, :width]
                ploop[1:2, r * LANES:r * LANES + width] = im[r:r + 1, :width]

    lane = lax.broadcasted_iota(jnp.int32, (1, LANES), 1)

    def finish():
        sums = jnp.sum(others[...], axis=0) / total_sites
        spread = jnp.where(lane < 2, -sums * sums, jnp.where(lane == 2, sums, 0.0))
        total = jnp.sum(spread, axis=1, keepdims=True)
        stats[...] = jnp.where(lane == 2, total, sums)[:, :3]

    for g in range(2):
        @pl.when(hi == middles[g])
        def _(g=g):
            parts = []
            for src in range(high):
                if src == middles[g]:
                    parts.append(take([send2[1, c] for c in range(12)], 2))
                    continue
                pltpu.make_async_copy(recv2.at[src], recv2.at[src], recv_sem2.at[src]).wait()
                parts.append(take([recv2[src, c] for c in range(12)], 2))
            left, right = whole(product(parts[:half])), whole(product(parts[half:]))
            terms = [cmul(left[i][j], right[j][i]) for i in range(3) for j in range(3)]
            re = functools.reduce(jnp.add, [x[0] for x in terms]) / 3.0
            im = functools.reduce(jnp.add, [x[1] for x in terms]) / 3.0
            row = jnp.zeros((1, LANES), jnp.float32)
            for k, value in enumerate((re, im, re * re + im * im)):
                value = jnp.sum(jnp.sum(value, axis=0, keepdims=True), axis=1, keepdims=True)
                row = jnp.where(lane == k, value, row)
            slot = (g * low + lo) * space + me_space
            mine[...] = row
            others[slot] = row

            def spread(step, carry):
                other = (me + step) % count
                pltpu.make_async_remote_copy(
                    src_ref=mine, dst_ref=others.at[slot], send_sem=send_sem3, recv_sem=recv_sem3,
                    device_id=(other // space, other % space), device_id_type=MESH,
                ).start()
                return carry

            lax.fori_loop(1, count, spread, 0, unroll=count <= 64)
            copies = []
            for k in range(half):
                owner = g * half + k
                real, imag = re[k * rows:(k + 1) * rows, :], im[k * rows:(k + 1) * rows, :]
                if owner == middles[g]:
                    place(real, imag)
                    continue
                outbox[k, 0] = real
                outbox[k, 1] = imag
                copy = pltpu.make_async_remote_copy(
                    src_ref=outbox.at[k], dst_ref=inbox, send_sem=send_sem4.at[k], recv_sem=recv_sem4,
                    device_id=(owner * low + lo, me_space), device_id_type=MESH,
                )
                copy.start()
                copies.append(copy)
            pltpu.make_async_copy(others.at[0:voices - 1], others.at[0:voices - 1], recv_sem3).wait()
            finish()
            for copy in copies:
                copy.wait_send()
            pltpu.make_async_copy(shadow, shadow, send_sem3).wait()

    @pl.when(jnp.logical_not(middle))
    def _():
        pltpu.make_async_copy(inbox, inbox, recv_sem4).wait()
        place(inbox[0], inbox[1])
        send_product(1).wait_send()
        pltpu.make_async_copy(others, others, recv_sem3).wait()
        finish()

    send_product(0).wait_send()
    for copy in sends1[0] + sends1[1]:
        copy.wait_send()


def on_device(tm, space, links):
    nt, sites = links.shape[3], links.shape[4]
    share = sites // tm
    unit = LANES * (8 // math.gcd(8, nt))
    padded = -(-share // unit) * unit
    rows = padded // LANES
    low = 1 << (tm.bit_length() - 1) // 2
    high = tm // low
    view = links.reshape(18, nt, tm, share)
    if padded != share:
        view = jnp.pad(view, ((0, 0), (0, 0), (0, 0), (0, padded - share)))
    view = view.reshape(18, nt, tm * rows, LANES).transpose(0, 2, 1, 3)
    view = view.reshape(18, high, low, rows * nt, LANES)
    band, part = high * rows, high // 2 * rows
    count = tm * space
    f32 = jnp.float32
    peers = max(low - 1, 1)
    ploop, stats = pl.pallas_call(
        functools.partial(kernel, tm, space, low, high, nt, rows, share, sites * space),
        out_shape=(jax.ShapeDtypeStruct((2, share), f32), jax.ShapeDtypeStruct((1, 3), f32)),
        in_specs=[pl.BlockSpec(memory_space=pl.ANY)],
        out_specs=(pl.BlockSpec(memory_space=pltpu.VMEM), pl.BlockSpec(memory_space=pltpu.VMEM)),
        scratch_shapes=[
            pltpu.VMEM((low, 18, band * nt, LANES), f32),
            pltpu.VMEM((peers, 2, 12, part, LANES), f32),
            pltpu.VMEM((low, 2, 12, part, LANES), f32),
            pltpu.VMEM((2, 12, part, LANES), f32),
            pltpu.VMEM((high, 12, part, LANES), f32),
            pltpu.VMEM((high // 2, 2, rows, LANES), f32),
            pltpu.VMEM((2, rows, LANES), f32),
            pltpu.VMEM((1, LANES), f32),
            pltpu.VMEM((2 * low * space, 1, LANES), f32),
            pltpu.VMEM((count - 1, 1, LANES), f32),
            pltpu.SemaphoreType.DMA((low,)),
            pltpu.SemaphoreType.DMA((peers, 2)),
            pltpu.SemaphoreType.DMA((peers, 2)),
            pltpu.SemaphoreType.DMA((2,)),
            pltpu.SemaphoreType.DMA((high,)),
            pltpu.SemaphoreType.DMA,
            pltpu.SemaphoreType.DMA,
            pltpu.SemaphoreType.DMA((high // 2,)),
            pltpu.SemaphoreType.DMA,
        ],
        compiler_params=pltpu.CompilerParams(collective_id=0, has_side_effects=True),
    )(view)
    return ploop, stats.reshape(3)


def solution(mesh):
    return jax.shard_map(
        functools.partial(on_device, mesh.shape["tm"], mesh.shape["space"]),
        mesh=mesh,
        in_specs=(P(None, None, None, "tm", "space"),),
        out_specs=(P(None, ("space", "tm")), P()),
        check_vma=False,
    )
```

```python
import functools
import math

import jax
import jax.numpy as jnp
from jax import lax
from jax.experimental import pallas as pl
from jax.experimental.pallas import tpu as pltpu
from jax.sharding import PartitionSpec as P

MESH = pl.DeviceIdType.MESH
LANES = 128


def xor(index, flip):
    out, bit = 0, 1
    while bit <= flip:
        digit = index // bit % 2
        out = out + (bit * (1 - digit) if flip & bit else bit * digit)
        bit *= 2
    return out + index // bit * bit


def cmul(a, b):
    return (a[0] * b[0] - a[1] * b[1], a[0] * b[1] + a[1] * b[0])


def times(left, right):
    out = []
    for row in left:
        new = []
        for k in range(3):
            terms = [cmul(row[j], right[j][k]) for j in range(3)]
            new.append((terms[0][0] + terms[1][0] + terms[2][0], terms[0][1] + terms[1][1] + terms[2][1]))
        out.append(new)
    return out


def whole(rows):
    first, second = rows
    third = []
    for k in range(3):
        i, j = (k + 1) % 3, (k + 2) % 3
        p, q = cmul(first[i], second[j]), cmul(first[j], second[i])
        third.append((p[0] - q[0], q[1] - p[1]))
    return [first, second, third]


def take(block, rows):
    return [[(block[i * 3 + j], block[(rows + i) * 3 + j]) for j in range(3)] for i in range(rows)]


def flat(rows):
    return [x[part] for part in range(2) for row in rows for x in row]


def product(parts):
    while len(parts) > 1:
        merged = [times(parts[n], whole(parts[n + 1])) for n in range(0, len(parts) - 1, 2)]
        parts = merged + parts[2 * len(merged):]
    return parts[0]


def kernel(tm, space, low, high, nt, rows, share, total_sites,
           links, ploop, stats,
           staged, send1, recv1, send2, recv2, outbox, inbox, mine, others, shadow,
           in_sem, send_sem1, recv_sem1, send_sem2, recv_sem2, send_sem3, recv_sem3, send_sem4, recv_sem4):
    me_tm, me_space = lax.axis_index("tm"), lax.axis_index("space")
    lo, hi = me_tm % low, me_tm // low
    me = me_tm * space + me_space
    count = tm * space
    band = high * rows
    half = high // 2
    part = half * rows
    near = hi // half
    far = 1 - near
    order = (far, near)
    middles = (half - 1, half)
    voices = 2 * low * space

    def chunk_copies(slot, target):
        return [
            pltpu.make_async_copy(
                links.at[:, h, target], staged.at[slot, :, pl.ds(h * rows * nt, rows * nt), :], in_sem.at[slot]
            )
            for h in range(high)
        ]

    barrier = pltpu.get_barrier_semaphore()

    def greet(other_tm, other_space):
        pl.semaphore_signal(barrier, inc=1, device_id=(other_tm, other_space), device_id_type=MESH)

    for step in range(1, low):
        greet(hi * low + (lo + step) % low, me_space)
    for step in range(1, space):
        greet(me_tm, (me_space + step) % space)
    middle = (hi >= middles[0]) & (hi <= middles[1])

    @pl.when(middle)
    def _():
        for step in range(1, high):
            greet((hi + step) % high * low + lo, me_space)

    @pl.when(jnp.logical_not(middle))
    def _():
        for h in middles:
            greet(h * low + lo, me_space)

    flips = [low - 1] + list(range(1, low - 1)) + [0] if low > 1 else [0]
    targets = [xor(lo, flip) for flip in flips]
    for slot, target in enumerate(targets):
        for copy in chunk_copies(slot, target):
            copy.start()

    def send_half(slot, turn):
        copy = pltpu.make_async_remote_copy(
            src_ref=send1.at[slot, order[turn]], dst_ref=recv1.at[lo, order[turn]],
            send_sem=send_sem1.at[slot, turn], recv_sem=recv_sem1.at[slot, turn],
            device_id=(hi * low + targets[slot], me_space), device_id_type=MESH,
        )
        copy.start()
        return copy

    sends1 = ([], [])
    for slot, target in enumerate(targets):
        pltpu.make_async_copy(staged.at[slot], staged.at[slot], in_sem.at[slot]).wait()

        def matrix(t, count_rows):
            block = {}
            for p in range(2):
                for i in range(count_rows):
                    for j in range(3):
                        block[(p * count_rows + i) * 3 + j] = staged[
                            slot, p * 9 + i * 3 + j, pl.ds(t, band, stride=nt), :
                        ]
            return take(block, count_rows)

        acc = matrix(0, 2)
        for t in range(1, nt):
            acc = times(acc, matrix(t, 3))
        own = slot == len(targets) - 1
        for c, value in enumerate(flat(acc)):
            for k in range(2):
                if own:
                    recv1[lo, k, c] = value[k * part:(k + 1) * part, :]
                else:
                    send1[slot, k, c] = value[k * part:(k + 1) * part, :]
        if slot == 0:
            @pl.when(middle)
            def _():
                pl.semaphore_wait(barrier, low - 1 + space - 1 + high - 1)

            @pl.when(jnp.logical_not(middle))
            def _():
                pl.semaphore_wait(barrier, low - 1 + space - 1 + 2)
        if not own:
            sends1[0].append(send_half(slot, 0))
        if slot == len(targets) - 2:
            sends1[1].extend(send_half(k, 1) for k in range(len(targets) - 1))

    def send_product(turn):
        return pltpu.make_async_remote_copy(
            src_ref=send2.at[turn], dst_ref=recv2.at[hi],
            send_sem=send_sem2.at[turn], recv_sem=recv_sem2.at[hi],
            device_id=((half - 1 + order[turn]) * low + lo, me_space), device_id_type=MESH,
        )

    for turn in range(2):
        for copy in sends1[turn]:
            copy.wait_recv()
        acc = product([take([recv1[src, order[turn], c] for c in range(12)], 2) for src in range(low)])
        for c, value in enumerate(flat(acc)):
            send2[turn, c] = value
        if turn == 0:
            send_product(0).start()

    @pl.when(jnp.logical_not(middle))
    def _():
        send_product(1).start()

    def place(re, im):
        for r in range(rows):
            width = min(LANES, share - r * LANES)
            if width > 0:
                ploop[0:1, r * LANES:r * LANES + width] = re[r:r + 1, :width]
                ploop[1:2, r * LANES:r * LANES + width] = im[r:r + 1, :width]

    lane = lax.broadcasted_iota(jnp.int32, (1, LANES), 1)

    def finish():
        sums = jnp.sum(others[...], axis=0) / total_sites
        spread = jnp.where(lane < 2, -sums * sums, jnp.where(lane == 2, sums, 0.0))
        total = jnp.sum(spread, axis=1, keepdims=True)
        stats[...] = jnp.where(lane == 2, total, sums)[:, :3]

    for g in range(2):
        @pl.when(hi == middles[g])
        def _(g=g):
            parts = []
            for src in range(high):
                if src == middles[g]:
                    parts.append(take([send2[1, c] for c in range(12)], 2))
                    continue
                pltpu.make_async_copy(recv2.at[src], recv2.at[src], recv_sem2.at[src]).wait()
                parts.append(take([recv2[src, c] for c in range(12)], 2))
            left, right = whole(product(parts[:half])), whole(product(parts[half:]))
            terms = [cmul(left[i][j], right[j][i]) for i in range(3) for j in range(3)]
            re = functools.reduce(jnp.add, [x[0] for x in terms]) / 3.0
            im = functools.reduce(jnp.add, [x[1] for x in terms]) / 3.0
            row = jnp.zeros((1, LANES), jnp.float32)
            for k, value in enumerate((re, im, re * re + im * im)):
                value = jnp.sum(jnp.sum(value, axis=0, keepdims=True), axis=1, keepdims=True)
                row = jnp.where(lane == k, value, row)
            slot = (g * low + lo) * space + me_space
            mine[...] = row
            others[slot] = row

            def spread(step, carry):
                other = (me + step) % count
                pltpu.make_async_remote_copy(
                    src_ref=mine, dst_ref=others.at[slot], send_sem=send_sem3, recv_sem=recv_sem3,
                    device_id=(other // space, other % space), device_id_type=MESH,
                ).start()
                return carry

            lax.fori_loop(1, count, spread, 0, unroll=count <= 64)
            copies = []
            for k in range(half):
                owner = g * half + k
                real, imag = re[k * rows:(k + 1) * rows, :], im[k * rows:(k + 1) * rows, :]
                if owner == middles[g]:
                    place(real, imag)
                    continue
                outbox[k, 0] = real
                outbox[k, 1] = imag
                copy = pltpu.make_async_remote_copy(
                    src_ref=outbox.at[k], dst_ref=inbox, send_sem=send_sem4.at[k], recv_sem=recv_sem4,
                    device_id=(owner * low + lo, me_space), device_id_type=MESH,
                )
                copy.start()
                copies.append(copy)
            pltpu.make_async_copy(others.at[0:voices - 1], others.at[0:voices - 1], recv_sem3).wait()
            finish()
            for copy in copies:
                copy.wait_send()
            pltpu.make_async_copy(shadow, shadow, send_sem3).wait()

    @pl.when(jnp.logical_not(middle))
    def _():
        pltpu.make_async_copy(inbox, inbox, recv_sem4).wait()
        place(inbox[0], inbox[1])
        send_product(1).wait_send()
        pltpu.make_async_copy(others, others, recv_sem3).wait()
        finish()

    send_product(0).wait_send()
    for copy in sends1[0] + sends1[1]:
        copy.wait_send()


def hand_out(ploop, stats, ploop_out, stats_out, sem_a, sem_b):
    first = pltpu.make_async_copy(ploop, ploop_out, sem_a)
    second = pltpu.make_async_copy(stats, stats_out, sem_b)
    first.start()
    second.start()
    first.wait()
    second.wait()


def on_device(tm, space, links):
    nt, sites = links.shape[3], links.shape[4]
    share = sites // tm
    unit = LANES * (8 // math.gcd(8, nt))
    padded = -(-share // unit) * unit
    rows = padded // LANES
    low = 1 << (tm.bit_length() - 1) // 2
    high = tm // low
    view = links.reshape(18, nt, tm, share)
    if padded != share:
        view = jnp.pad(view, ((0, 0), (0, 0), (0, 0), (0, padded - share)))
    view = view.reshape(18, nt, tm * rows, LANES).transpose(0, 2, 1, 3)
    view = view.reshape(18, high, low, rows * nt, LANES)
    view = pltpu.with_memory_space_constraint(view, pltpu.HBM)
    band, part = high * rows, high // 2 * rows
    count = tm * space
    f32 = jnp.float32
    peers = max(low - 1, 1)
    ploop, stats = pl.pallas_call(
        functools.partial(kernel, tm, space, low, high, nt, rows, share, sites * space),
        out_shape=(jax.ShapeDtypeStruct((2, share), f32), jax.ShapeDtypeStruct((1, 3), f32)),
        in_specs=[pl.BlockSpec(memory_space=pltpu.HBM)],
        out_specs=(pl.BlockSpec(memory_space=pltpu.VMEM), pl.BlockSpec(memory_space=pltpu.VMEM)),
        scratch_shapes=[
            pltpu.VMEM((low, 18, band * nt, LANES), f32),
            pltpu.VMEM((peers, 2, 12, part, LANES), f32),
            pltpu.VMEM((low, 2, 12, part, LANES), f32),
            pltpu.VMEM((2, 12, part, LANES), f32),
            pltpu.VMEM((high, 12, part, LANES), f32),
            pltpu.VMEM((high // 2, 2, rows, LANES), f32),
            pltpu.VMEM((2, rows, LANES), f32),
            pltpu.VMEM((1, LANES), f32),
            pltpu.VMEM((2 * low * space, 1, LANES), f32),
            pltpu.VMEM((count - 1, 1, LANES), f32),
            pltpu.SemaphoreType.DMA((low,)),
            pltpu.SemaphoreType.DMA((peers, 2)),
            pltpu.SemaphoreType.DMA((peers, 2)),
            pltpu.SemaphoreType.DMA((2,)),
            pltpu.SemaphoreType.DMA((high,)),
            pltpu.SemaphoreType.DMA,
            pltpu.SemaphoreType.DMA,
            pltpu.SemaphoreType.DMA((high // 2,)),
            pltpu.SemaphoreType.DMA,
        ],
        compiler_params=pltpu.CompilerParams(collective_id=0, has_side_effects=True, vmem_limit_bytes=24 << 20),
    )(view)
    ploop, stats = pl.pallas_call(
        hand_out,
        out_shape=(jax.ShapeDtypeStruct((2, share), f32), jax.ShapeDtypeStruct((1, 3), f32)),
        in_specs=[pl.BlockSpec(memory_space=pltpu.VMEM)] * 2,
        out_specs=[pl.BlockSpec(memory_space=pltpu.HBM)] * 2,
        scratch_shapes=[pltpu.SemaphoreType.DMA, pltpu.SemaphoreType.DMA],
        compiler_params=pltpu.CompilerParams(vmem_limit_bytes=1 << 20),
    )(ploop, stats)
    return ploop, stats.reshape(3)


def solution(mesh):
    return jax.shard_map(
        functools.partial(on_device, mesh.shape["tm"], mesh.shape["space"]),
        mesh=mesh,
        in_specs=(P(None, None, None, "tm", "space"),),
        out_specs=(P(None, ("space", "tm")), P()),
        check_vma=False,
    )
```
